256 devices in a mesh: dp: 32 (over x, z), section: 8 (over y, core).
Axes of the slice: x: 4, y: 4, z: 8, core: 2. Of those that a mesh axis runs over, the one named last changes fastest.
Arguments:
- activations: bfloat16 [8, 64, 512, 4096], P('section', 'dp'), may hold values from -16 to 16
- out_grads: bfloat16 [8, 64, 512, 1024], P('section', 'dp'), may hold values from -16 to 16
- lengths: int32 [64], P('dp'), may hold values from 64 to 512, as said below
Outputs:
- mean_grad: bfloat16 [8, 4096, 1024], P('section', 'dp')
- norm_ratio: float32 [64], P('dp')
The draws below stay inside these ranges and needn't reach their ends.
Inputs may be any that keep to these rules, and one draw needn't show every extreme that they name: Example e's first lengths[e] token slots are real, the rest padding; some example fills all 512 slots.
All inputs are finite; a program needn't handle non-finite values.
Results may differ from the reference program's by a relative error of at most 0.015.
Values may be sent and summed in bfloat16 or wider, within the bound.
No kernel may reach another device: no remote copies, remote signals or barrier semaphores. Data moves between devices by JAX's collectives and lax.ppermute only.
A program may use at most 128 MiB of HBM per device.

```python
import math
import jax
import jax.numpy as jnp
from jax import lax

D = 4096
KV = 1024
SEQ = 512
EX_DEV = 2
LAYERS = 8
EXAMPLES = 64
N_DP = 32


def feature_values(key, shape):
    base_key, scale_key, common_key, row_key = jax.random.split(key, 4)
    values = jax.random.normal(base_key, shape, jnp.float32)
    layer_scale = jax.random.uniform(scale_key, (shape[0], shape[1], 1, 1), jnp.float32, 0.5, 2.0)
    return values * layer_scale


def example_order(key):
    length_key, ranking_key = jax.random.split(jax.random.fold_in(key, 37))
    ranking = jax.random.permutation(ranking_key, EXAMPLES)
    return (length_key, ranking)


def draw_activations(key, part):
    values = feature_values(jax.random.fold_in(key, 11), (LAYERS, EXAMPLES, SEQ, D))
    return jnp.clip(values, -16.0, 16.0).astype(jnp.bfloat16)


def draw_out_grads(key, part):
    values = feature_values(jax.random.fold_in(key, 23), (LAYERS, EXAMPLES, SEQ, KV))
    length_key, ranking = example_order(key)
    log_factor = jax.random.uniform(jax.random.fold_in(key, 41), (EXAMPLES,), jnp.float32, jnp.log(0.05), jnp.log(2.0))
    example_factor = jnp.exp(log_factor)
    example_factor = example_factor.at[ranking[0]].set(2.0).at[ranking[1]].set(0.05)
    values = values * example_factor[None, :, None, None]
    return jnp.clip(values, -16.0, 16.0).astype(jnp.bfloat16)


def draw_lengths(key, part):
    length_key, ranking = example_order(key)
    values = jax.random.randint(length_key, (EXAMPLES,), SEQ // 8, SEQ + 1)
    values = values.at[ranking[0]].set(SEQ).at[ranking[1]].set(SEQ // 8)
    return values.astype(jnp.int32)


def setup_inputs(seed: int = 0) -> dict:
    keys = jax.random.split(jax.random.key(seed), 4)
    return {
        "activations": draw_activations(jax.random.fold_in(keys[3], 71), 0),
        "out_grads": draw_out_grads(jax.random.fold_in(keys[3], 71), 0),
        "lengths": draw_lengths(jax.random.fold_in(keys[3], 71), 0),
    }


def example_norm(operands):
    example_acts, example_grads = operands
    act_rows = example_acts.astype(jnp.float32)
    grad_values = example_grads.astype(jnp.float32)
    act_gram = jnp.dot(act_rows, act_rows.T, precision=lax.Precision.HIGHEST)
    grad_gram = jnp.dot(grad_values, grad_values.T, precision=lax.Precision.HIGHEST)
    return jnp.sum(act_gram * grad_gram)

def layer_norm_list(operands):
    return lax.map(example_norm, operands)

def reference(activations, out_grads, lengths):
    clip_bound = 0.5 * math.sqrt(float(LAYERS * SEQ * D * KV))
    positions = jnp.arange(SEQ, dtype=jnp.int32)
    token_keep = (positions[None, :] < lengths[:, None]).astype(jnp.bfloat16)
    masked = out_grads * token_keep[None, :, :, None]
    layer_norms = lax.map(layer_norm_list, (activations, masked))
    norm_total = lax.optimization_barrier(jnp.sum(layer_norms, axis=0))
    norm_ratio = jnp.sqrt(norm_total) / clip_bound
    clip_factor = 1.0 / jnp.maximum(norm_ratio, 1.0)

    def layer_grad(operands):
        layer_acts, layer_grads = operands
        scaled = (clip_factor[:, None, None] * layer_grads).astype(jnp.bfloat16)
        act_groups = layer_acts.reshape(N_DP, EX_DEV * SEQ, D)
        scaled_groups = scaled.reshape(N_DP, EX_DEV * SEQ, KV)

        def add_group(running, group):
            group_acts, group_scaled = group
            partial_sum = lax.dot_general(group_acts, group_scaled, (((0,), (0,)), ((), ())), preferred_element_type=jnp.float32)
            partial_sum = partial_sum.astype(jnp.bfloat16)
            return (running + partial_sum.astype(jnp.float32), None)
        summed, _ = lax.scan(add_group, jnp.zeros((D, KV), jnp.float32), (act_groups, scaled_groups))
        return (summed / EXAMPLES).astype(jnp.bfloat16)
    mean_grad = lax.map(layer_grad, (activations, masked))
    return (mean_grad, norm_ratio)
```

```python
import functools
import math

import jax
import jax.numpy as jnp
from jax import lax
from jax.experimental import pallas as pl
from jax.experimental.pallas import tpu as pltpu
from jax.sharding import Mesh
from jax.sharding import PartitionSpec as P

DP = ("dp_0", "dp_1")
LANES = 128
NORM_STEPS = 4
WHOLE = pl.BlockSpec(memory_space=pltpu.VMEM)


def bf(v):
    return v.astype(jnp.bfloat16)


def f32(v):
    return v.astype(jnp.float32)


def in_hbm(v):
    return pltpu.with_memory_space_constraint(v, pltpu.HBM)


def in_vmem(v):
    return pltpu.with_memory_space_constraint(v, pltpu.VMEM)


def section_total(own):
    count = lax.axis_size("section")
    total = own
    for level in range(count.bit_length() - 1):
        total = total + lax.ppermute(total, "section", [(i, i ^ 1 << level) for i in range(count)])
    return total


def shift(block, axis, step):
    count = lax.axis_size(axis)
    return lax.ppermute(block, axis, [(i, (i + step) % count) for i in range(count)])


def row_products(left, right):
    return lax.dot_general(left, right, (((1,), (1,)), ((), ())), preferred_element_type=jnp.float32)


def norm_kernel(len_ref, act_ref, grad_ref, norm_ref, top_ref, low_ref):
    j = pl.program_id(0)
    examples, seq, _ = act_ref.shape
    half = seq // 2
    for e in range(examples):
        acts = act_ref[e]
        top = row_products(acts[:half], acts)
        low = row_products(acts[half:], acts[half:])

        @pl.when(j == 0)
        def _():
            top_ref[e] = top
            low_ref[e] = low

        @pl.when(j > 0)
        def _():
            top_ref[e] += top
            low_ref[e] += low

    @pl.when(j == pl.num_programs(0) - 1)
    def _():
        row = lax.broadcasted_iota(jnp.int32, (half, seq), 0)
        col = lax.broadcasted_iota(jnp.int32, (half, seq), 1)
        for e in range(examples):
            grads = grad_ref[e]
            size = len_ref[e]
            top = row_products(grads[:half], grads) * top_ref[e]
            low = row_products(grads[half:], grads[half:]) * low_ref[e]
            top = jnp.where((row < size) & (col < size), top, 0.0)
            inner = (row[:, :half] + half < size) & (col[:, :half] + half < size)
            low = jnp.where(inner, low, 0.0)
            total = jnp.sum(top[:, :half]) + 2.0 * jnp.sum(top[:, half:]) + jnp.sum(low)
            norm_ref[e] = jnp.full(norm_ref.shape[1:], total, jnp.float32)


def example_norms(acts, grads, lengths):
    examples, seq, width = acts.shape
    key = grads.shape[2]
    tile = width // NORM_STEPS
    half = seq // 2
    return pl.pallas_call(
        norm_kernel,
        grid=(NORM_STEPS,),
        in_specs=[
            pl.BlockSpec(memory_space=pltpu.SMEM),
            pl.BlockSpec((examples, seq, tile), lambda j: (0, 0, j)),
            pl.BlockSpec((examples, seq, key), lambda j: (0, 0, 0)),
        ],
        out_specs=WHOLE,
        out_shape=pltpu.VMEM((examples, 8, LANES), jnp.float32),
        scratch_shapes=[
            pltpu.VMEM((examples, half, seq), jnp.float32),
            pltpu.VMEM((examples, half, half), jnp.float32),
        ],
        compiler_params=pltpu.CompilerParams(
            dimension_semantics=("arbitrary",), vmem_limit_bytes=28 << 20
        ),
        name="example_norms",
    )(lengths, in_hbm(acts), in_hbm(grads))


def scale_kernel(bound, len_ref, total_ref, grad_ref, flip_ref):
    examples, seq, _ = grad_ref.shape
    for e in range(examples):
        clip = 1.0 / jnp.maximum(jnp.sqrt(total_ref[e]) / bound, 1.0)
        grads = f32(grad_ref[e])
        token = lax.broadcasted_iota(jnp.int32, grads.shape, 0)
        scaled = jnp.where(token < len_ref[e], grads, 0.0) * clip[:1, :1]
        flip_ref[:, e * seq : (e + 1) * seq] = bf(scaled).T


def scaled_rows(grads, total, lengths, bound):
    examples, seq, key = grads.shape
    return pl.pallas_call(
        functools.partial(scale_kernel, bound),
        in_specs=[pl.BlockSpec(memory_space=pltpu.SMEM), WHOLE, WHOLE],
        out_specs=WHOLE,
        out_shape=pltpu.VMEM((key, examples * seq), jnp.bfloat16),
        compiler_params=pltpu.CompilerParams(vmem_limit_bytes=20 << 20),
        name="scaled_rows",
    )(lengths, in_vmem(total), grads)


def pieces(acts, flipped, ids, per_step, splits, name):
    examples, seq, _ = acts.shape
    key = flipped.shape[0]
    steps = sum(splits)

    def kernel(ids_ref, flip_ref, *refs):
        j = pl.program_id(0)
        strips, outs = refs[:per_step], refs[per_step:]
        block = jnp.concatenate([s[...].reshape(examples * seq, LANES) for s in strips], 1)
        value = bf(jnp.dot(flip_ref[...], block, preferred_element_type=jnp.float32))
        start = 0
        for out, size in zip(outs, splits):

            @pl.when((j >= start) & (j < start + size))
            def _(out=out, start=start):
                for q in range(per_step):
                    out[(j - start) * per_step + q] = value[:, q * LANES : (q + 1) * LANES]

            start += size

    strip = lambda q: pl.BlockSpec((examples, seq, LANES), lambda j, ids: (0, 0, ids[j * per_step + q]))
    return pl.pallas_call(
        kernel,
        grid_spec=pltpu.PrefetchScalarGridSpec(
            num_scalar_prefetch=1,
            grid=(steps,),
            in_specs=[WHOLE] + [strip(q) for q in range(per_step)],
            out_specs=[WHOLE] * len(splits),
        ),
        out_shape=[pltpu.VMEM((size * per_step, key, LANES), jnp.bfloat16) for size in splits],
        compiler_params=pltpu.CompilerParams(
            dimension_semantics=("arbitrary",), vmem_limit_bytes=16 << 20
        ),
        name=name,
    )(ids, in_vmem(flipped), *[in_hbm(acts)] * per_step)


def call(kernel, outs, name, *args):
    return pl.pallas_call(
        kernel,
        in_specs=[WHOLE] * len(args),
        out_specs=[WHOLE] * len(outs),
        out_shape=[pltpu.VMEM(shape, dtype) for shape, dtype in outs],
        compiler_params=pltpu.CompilerParams(vmem_limit_bytes=8 << 20),
        name=name,
    )(*[in_vmem(a) for a in args])


def plus(stored, at, size, got):
    def kernel(stored_ref, got_ref, out_ref):
        out_ref[...] = bf(f32(stored_ref[at : at + size]) + f32(got_ref[...]))

    return call(kernel, [(got.shape, got.dtype)], "plus", stored, got)[0]


def two_way(acts, flipped, axis, block_id, size):
    count = lax.axis_size(axis)
    far = count // 2
    index = lax.axis_index(axis)
    plan = []
    for slot in range(count - 1):
        for step in (1, -1):
            half = slot % 2 if step == 1 else 1 - slot % 2
            hops = far - (slot + 1) // 2
            plan.append((step, half, hops))
    ids = [jnp.stack(block_id((index + s * h) % count, half)) for s, half, h in plan]
    own = [jnp.stack(block_id(index, half)) for half in (0, 1)]
    lead = pieces(acts, flipped, jnp.concatenate(ids[:2]), size, [1, 1], "lead")
    next_ids, lead = lax.optimization_barrier((jnp.concatenate(ids[2:4]), lead))
    sent = {}
    for (step, half, _), out in zip(plan[:2], lead):
        sent[step, half] = shift(out, axis, step)
    second = pieces(acts, flipped, next_ids, size, [1, 1], "second")
    rest_ids, second = lax.optimization_barrier((jnp.concatenate(ids[4:] + own), second))
    for (step, half, _), out in zip(plan[2:4], second):
        sent[step, half] = shift(out, axis, step)
    stored = pieces(acts, flipped, rest_ids, size, [len(plan) - 2], "rest")[0]
    for k, (step, half, _) in enumerate(plan[4:]):
        sent[step, half] = shift(plus(stored, k * size, size, sent[step, half]), axis, step)
    at = (len(plan) - 4) * size
    return stored, at, [[sent[step, half] for step in (1, -1)] for half in (0, 1)]


def x_first(acts, flipped, samples):
    nx, nz = lax.axis_size("dp_0"), lax.axis_size("dp_1")
    key = flipped.shape[0]
    here = lax.axis_index("dp_1")
    order = [[4, 3, 1, 2], [-3, -1, -2, 0]]
    block_id = lambda t, half: [t * nz + (here + d) % nz for d in order[half]]
    stored, at, got = two_way(acts, flipped, "dp_0", block_id, 4)

    def rows_kernel(stored_ref, a1, a2, b1, b2, far_1, far_2, near_1, near_2, keep):
        def row(half, k):
            one, two = ((a1, a2), (b1, b2))[half]
            value = f32(stored_ref[at + 4 * half + k])
            return bf(value + f32(one[k]) + f32(two[k]))

        opposite = row(0, 0)
        far_1[...] = opposite[: key // 2]
        far_2[...] = opposite[key // 2 :]
        near_1[0] = row(0, 1)
        near_1[1] = row(0, 2)
        near_2[0] = row(1, 0)
        near_2[1] = row(1, 1)
        keep[0] = row(0, 3)
        keep[1] = row(1, 2)
        keep[2] = row(1, 3)

    block = lambda n: ((n, key, LANES), jnp.bfloat16)
    part = ((key // 2, LANES), jnp.bfloat16)
    outs = [part, part, block(2), block(2), block(3)]
    far_1, far_2, near_1, near_2, keep = call(rows_kernel, outs, "rows", stored, *got[0], *got[1])
    near = [shift(near_1, "dp_1", 1), shift(near_2, "dp_1", -1)]
    far = [shift(far_1, "dp_1", 2), shift(far_2, "dp_1", -2)]
    last = []
    for side, step in enumerate((2, -2)):

        def pass_kernel(keep_ref, near_ref, far_ref, out_ref, side=side):
            for k in (0, 1):
                cut = slice(k * key // 2, (k + 1) * key // 2)
                value = f32(keep_ref[side, cut]) + f32(near_ref[0, cut])
                if k == side:
                    value = value + f32(far_ref[...])
                out_ref[cut] = bf(value)

        out = call(pass_kernel, [((key, LANES), jnp.bfloat16)], "pass", keep, near[side], far[side])
        last.append(shift(out[0], "dp_1", step))

    def end_kernel(keep_ref, near_1, near_2, last_1, last_2, out_ref):
        value = f32(keep_ref[2]) + f32(near_1[1]) + f32(near_2[1])
        value = value + f32(last_1[...]) + f32(last_2[...])
        out_ref[...] = bf(value.T / samples)

    return call(end_kernel, [((LANES, key), jnp.bfloat16)], "end", keep, *near, *last)[0]


def z_first(acts, flipped, samples):
    nx, nz = lax.axis_size("dp_0"), lax.axis_size("dp_1")
    key = flipped.shape[0]
    here = lax.axis_index("dp_0")
    order = [[2, 1], [-1, 0]]
    block_id = lambda t, half: [(here + d) % nx * nz + t for d in order[half]]
    stored, at, got = two_way(acts, flipped, "dp_1", block_id, 2)

    def rows_kernel(stored_ref, a1, a2, b1, b2, out_1, out_2, out_3, keep):
        for k, out in enumerate((out_1, out_2, out_3, keep)):
            one, two = (a1, a2) if k < 2 else (b1, b2)
            out[...] = bf(f32(stored_ref[at + k]) + f32(one[k % 2]) + f32(two[k % 2]))

    block = ((key, LANES), jnp.bfloat16)
    *outs, keep = call(rows_kernel, [block] * 4, "rows", stored, *got[0], *got[1])
    moved = [shift(out, "dp_0", d) for out, d in zip(outs, (2, 1, -1))]

    def end_kernel(keep_ref, one, two, three, out_ref):
        value = f32(keep_ref[...]) + f32(one[...]) + f32(two[...]) + f32(three[...])
        out_ref[...] = bf(value.T / samples)

    return call(end_kernel, [((LANES, key), jnp.bfloat16)], "end", keep, *moved)[0]


def on_device(activations, out_grads, lengths):
    layer_count, example_count, seq_len, model_width = activations.shape
    key_width = out_grads.shape[3]
    total_layers = layer_count * lax.axis_size("section")
    clip_bound = 0.5 * math.sqrt(float(total_layers * seq_len * model_width * key_width))
    acts, grads = activations[0], out_grads[0]
    total = section_total(example_norms(acts, grads, lengths))
    flipped = scaled_rows(grads, total, lengths, clip_bound)
    samples = float(lax.axis_size(DP) * example_count)
    first = functools.partial(x_first, samples=samples)
    second = functools.partial(z_first, samples=samples)
    mean = lax.cond(lax.axis_index("section") % 2 == 0, first, second, acts, flipped)
    norm_ratio = jnp.sqrt(total[:, 0, 0]) / clip_bound
    return (mean[None], norm_ratio)


def solution(mesh):
    torus = Mesh(mesh.devices.reshape(4, 8, mesh.shape["section"]), ("dp_0", "dp_1", "section"))
    return jax.shard_map(
        on_device,
        mesh=torus,
        in_specs=(P("section", DP, None, None), P("section", DP, None, None), P(DP)),
        out_specs=(P("section", DP, None), P(DP)),
        check_vma=False,
    )
```

```python
import functools
import math

import jax
import jax.numpy as jnp
from jax import lax
from jax.experimental import pallas as pl
from jax.experimental.pallas import tpu as pltpu
from jax.sharding import Mesh
from jax.sharding import PartitionSpec as P


DP = ("dp_0", "dp_1")
LANES = 128
NORM_STEPS = 4
CHUNK = 256
WHOLE = pl.BlockSpec(memory_space=pltpu.VMEM)


def bf(v):
    return v.astype(jnp.bfloat16)


def f32(v):
    return v.astype(jnp.float32)


def in_hbm(v):
    return pltpu.with_memory_space_constraint(v, pltpu.HBM)


def in_vmem(v):
    return pltpu.with_memory_space_constraint(v, pltpu.VMEM)


def partner_sum(own, level, *order):
    count = lax.axis_size("section")
    moved = lax.ppermute(own, "section", [(i, i ^ 1 << level) for i in range(count)])

    def kernel(own_ref, moved_ref, *refs):
        refs[-1][...] = own_ref[...] + moved_ref[...]

    return call(kernel, [(own.shape, own.dtype)], own, moved, *order)[0]


def chunks(total, body):
    def step(i, _):
        body(pl.ds(pl.multiple_of(i * CHUNK, CHUNK), CHUNK))
        return 0

    lax.fori_loop(0, total // CHUNK, step, 0)


def shift(block, axis, step):
    count = lax.axis_size(axis)
    return lax.ppermute(block, axis, [(i, (i + step) % count) for i in range(count)])


def row_products(left, right):
    return lax.dot_general(left, right, (((1,), (1,)), ((), ())), preferred_element_type=jnp.float32)


def norm_kernel(len_ref, act_ref, grad_ref, norm_ref, top_ref, low_ref):
    j = pl.program_id(0)
    examples, seq, _ = act_ref.shape
    half = seq // 2
    first = j == 0

    def gram(e, _):
        acts = act_ref[e]
        top = row_products(acts[:half], acts)
        low = row_products(acts[half:], acts[half:])
        top_ref[e] = top + jnp.where(first, 0.0, top_ref[e])
        low_ref[e] = low + jnp.where(first, 0.0, low_ref[e])
        return 0

    lax.fori_loop(0, examples, gram, 0)

    def finish(e, _):
        row = lax.broadcasted_iota(jnp.int32, (half, seq), 0)
        col = lax.broadcasted_iota(jnp.int32, (half, seq), 1)
        grads = grad_ref[e]
        size = len_ref[e]
        top = row_products(grads[:half], grads) * top_ref[e]
        low = row_products(grads[half:], grads[half:]) * low_ref[e]
        top = jnp.where((row < size) & (col < size), top, 0.0)
        inner = (row[:, :half] + half < size) & (col[:, :half] + half < size)
        low = jnp.where(inner, low, 0.0)
        total = jnp.sum(top[:, :half]) + 2.0 * jnp.sum(top[:, half:]) + jnp.sum(low)
        norm_ref[e] = jnp.full(norm_ref.shape[1:], total, jnp.float32)
        return 0

    @pl.when(j == pl.num_programs(0) - 1)
    def _():
        lax.fori_loop(0, examples, finish, 0)


def example_norms(acts, grads, lengths):
    examples, seq, width = acts.shape
    key = grads.shape[2]
    tile = width // NORM_STEPS
    half = seq // 2
    return pl.pallas_call(
        norm_kernel,
        grid=(NORM_STEPS,),
        in_specs=[
            pl.BlockSpec(memory_space=pltpu.SMEM),
            pl.BlockSpec((examples, seq, tile), lambda j: (0, 0, j)),
            pl.BlockSpec((examples, seq, key), lambda j: (0, 0, 0)),
        ],
        out_specs=WHOLE,
        out_shape=pltpu.VMEM((examples, 8, LANES), jnp.float32),
        scratch_shapes=[
            pltpu.VMEM((examples, half, seq), jnp.float32),
            pltpu.VMEM((examples, half, half), jnp.float32),
        ],
        compiler_params=pltpu.CompilerParams(
            dimension_semantics=("arbitrary",), vmem_limit_bytes=28 << 20
        ),
        name="example_norms",
    )(lengths, in_hbm(acts), in_hbm(grads))


def on_chip(acts, order):
    def kernel(acts_ref, order_ref, out_ref, tile_ref, sem):
        tile_ref[...] = jnp.zeros_like(tile_ref)
        copy = pltpu.make_async_copy(acts_ref, out_ref, sem)
        copy.start()
        copy.wait()

    return pl.pallas_call(
        kernel,
        in_specs=[pl.BlockSpec(memory_space=pltpu.HBM), WHOLE],
        out_specs=[WHOLE, WHOLE],
        out_shape=[
            pltpu.VMEM(acts.shape, acts.dtype),
            pltpu.VMEM((8, LANES), jnp.float32),
        ],
        scratch_shapes=[pltpu.SemaphoreType.DMA],
        compiler_params=pltpu.CompilerParams(vmem_limit_bytes=2 << 20),
        name="on_chip",
    )(in_hbm(acts), in_vmem(order))


def masked_rows(grads, lengths, order):
    examples, seq, key = grads.shape

    def kernel(len_ref, grad_ref, order_ref, flip_ref, tile_ref):
        tile_ref[...] = jnp.zeros_like(tile_ref)

        def turn(e, _):
            token = lax.broadcasted_iota(jnp.int32, (seq, key), 0)
            masked = jnp.where(token < len_ref[e], f32(grad_ref[e]), 0.0)
            flip_ref[:, pl.ds(pl.multiple_of(e * seq, seq), seq)] = bf(masked).T
            return 0

        lax.fori_loop(0, examples, turn, 0)

    return pl.pallas_call(
        kernel,
        in_specs=[pl.BlockSpec(memory_space=pltpu.SMEM), WHOLE, WHOLE],
        out_specs=[WHOLE, WHOLE],
        out_shape=[
            pltpu.VMEM((key, examples * seq), jnp.bfloat16),
            pltpu.VMEM((8, LANES), jnp.float32),
        ],
        compiler_params=pltpu.CompilerParams(vmem_limit_bytes=16 << 20),
        name="masked_rows",
    )(lengths, grads, in_vmem(order))


def clipped_rows(flipped, total, bound):
    examples = total.shape[0]
    seq = flipped.shape[1] // examples

    def kernel(total_ref, flip_ref, out_ref, ratio_ref):
        clips = []
        for e in range(examples):
            ratio = jnp.sqrt(total_ref[e]) / bound
            ratio_ref[e] = ratio[0, 0]
            clips.append((1.0 / jnp.maximum(ratio, 1.0))[:1, :1])

        def body(rows):
            for e in range(examples):
                part = (rows, slice(e * seq, (e + 1) * seq))
                out_ref[part] = bf(f32(flip_ref[part]) * clips[e])

        chunks(flipped.shape[0], body)

    return pl.pallas_call(
        kernel,
        in_specs=[WHOLE, WHOLE],
        out_specs=[WHOLE, pl.BlockSpec(memory_space=pltpu.SMEM)],
        out_shape=[
            pltpu.VMEM(flipped.shape, flipped.dtype),
            jax.ShapeDtypeStruct((examples,), jnp.float32),
        ],
        compiler_params=pltpu.CompilerParams(vmem_limit_bytes=8 << 20),
        name="clipped_rows",
    )(in_vmem(total), in_vmem(flipped))


def pieces(acts, flipped, ids, outs, step, order):
    examples, seq, _ = acts.shape
    key = flipped.shape[0]

    def kernel(acts_ref, flip_ref, *refs):
        refs = refs[len(order) :]
        refs[-1][...] = jnp.zeros_like(refs[-1])
        blocks = ids()

        def strip(k):
            cols = pl.ds(pl.multiple_of(blocks[k] * LANES, LANES), LANES)
            return acts_ref[:, :, cols].reshape(examples * seq, LANES)

        places = [(out, at) for out, size in zip(refs[:-1], outs) for at in range(size)]

        def rows_of(i, _):
            rows = pl.ds(pl.multiple_of(i * step, step), step)
            for first in range(0, len(places), 4):
                some = range(first, min(first + 4, len(places)))
                block = jnp.concatenate([strip(k) for k in some], 1)
                value = jnp.dot(flip_ref[rows, :], block, preferred_element_type=jnp.float32)
                for q, k in enumerate(some):
                    out, at = places[k]
                    out[at, rows] = bf(value[:, q * LANES : (q + 1) * LANES])
            return 0

        lax.fori_loop(0, key // step, rows_of, 0)

    return pl.pallas_call(
        kernel,
        in_specs=[WHOLE] * (2 + len(order)),
        out_specs=[WHOLE] * (len(outs) + 1),
        out_shape=[pltpu.VMEM((size, key, LANES), jnp.bfloat16) for size in outs]
        + [pltpu.VMEM((8, LANES), jnp.float32)],
        compiler_params=pltpu.CompilerParams(vmem_limit_bytes=12 << 20),
        name="terms",
    )(*[in_vmem(v) for v in (acts, flipped, *order)])


def call(kernel, outs, *args, space=pltpu.VMEM):
    return pl.pallas_call(
        kernel,
        in_specs=[WHOLE] * len(args),
        out_specs=[WHOLE] * len(outs),
        out_shape=[space(shape, dtype) for shape, dtype in outs],
        compiler_params=pltpu.CompilerParams(vmem_limit_bytes=8 << 20),
    )(*[in_vmem(a) for a in args])


def plus(stored, got, skip=0):
    def kernel(stored_ref, got_ref, out_ref, order_ref):
        order_ref[...] = jnp.zeros_like(order_ref)

        def body(rows):
            for k in range(out_ref.shape[0]):
                out_ref[k, rows] = bf(f32(stored_ref[k, rows]) + f32(got_ref[skip + k, rows]))

        chunks(out_ref.shape[1], body)

    outs = [(stored.shape, stored.dtype), ((8, LANES), jnp.float32)]
    return call(kernel, outs, stored, got)


def two_way(acts, flipped, axis, block_id, size):
    count = lax.axis_size(axis)
    far = count // 2
    sent, order = {}, []
    for slot in range(count - 1):
        routes = [(step, slot % 2 if step == 1 else 1 - slot % 2) for step in (1, -1)]
        hops = far - (slot + 1) // 2
        wanted, outs = [(step * hops, half) for step, half in routes], [size, size]
        if slot == count - 2:
            wanted, outs = wanted + [(0, 0), (0, 1)], outs + [2 * size]

        def ids(wanted=wanted):
            index = lax.axis_index(axis)
            return [k for away, half in wanted for k in block_id((index + away) % count, half)]

        *terms, tile = pieces(acts, flipped, ids, outs, 256, order)
        order = [tile]
        for route, term in zip(routes, terms):
            if slot > 1:
                term, tile = plus(term, sent[route])
                order.append(tile)
            sent[route] = shift(term, axis, route[0])
    return terms[2], [[sent[step, half] for step in (1, -1)] for half in (0, 1)]


def x_first(acts, flipped, samples):
    nx, nz = lax.axis_size("dp_0"), lax.axis_size("dp_1")
    key = flipped.shape[0]
    block = ((key, LANES), jnp.bfloat16)

    offsets = {(0, 0): [4, 3], (0, 1): [1, -3], (1, 0): [-1, 2], (1, 1): [-2, 0]}
    steps = (1, -1)

    def terms(*wanted, order):
        def ids():
            x, z = lax.axis_index("dp_0"), lax.axis_index("dp_1")
            return [
                (x + away) % nx * nz + (z + d) % nz
                for parts in wanted
                for batch, half, away in parts
                for d in offsets[batch, half]
            ]

        outs = [2 * len(parts) for parts in wanted]
        return pieces(acts, flipped, ids, outs, 256, order)

    lead = {1: 0, -1: 1}
    far = lambda batch, step: (batch, lead[step], 2 * step)
    lag = lambda batch, step: (batch, 1 - lead[step], step)
    near = lambda batch, step: (batch, lead[step], step)
    own = lambda batch: [(batch, 0, 0), (batch, 1, 0)]

    def send(blocks):
        return {step: shift(block, "dp_0", step) for step, block in zip(steps, blocks)}

    def add(blocks, got, skip):
        outs = [plus(block, got[step], skip) for step, block in zip(steps, blocks)]
        return [out for out, _ in outs], [tile for _, tile in outs]

    def row(refs, k, rows):
        stored, a1, a2, b1, b2 = refs
        one, two = (a1, a2) if k < 2 else (b1, b2)
        return bf(f32(stored[k, rows]) + f32(one[k % 2, rows]) + f32(two[k % 2, rows]))

    def outer_kernel(*refs):
        four, pair, minus_three = refs[5:]

        def body(rows):
            four[rows] = row(refs[:5], 0, rows)
            pair[0, rows] = row(refs[:5], 1, rows)
            pair[1, rows] = row(refs[:5], 2, rows)
            minus_three[rows] = row(refs[:5], 3, rows)

        chunks(key, body)

    def inner_kernel(*refs):
        outs = refs[5:]

        def body(rows):
            for k, out in enumerate(outs):
                out[rows] = row(refs[:5], k, rows)

        chunks(key, body)

    def passed(step, kept, got):
        def kernel(kept_ref, got_ref, out_ref):
            def body(rows):
                came = got_ref[rows] if got_ref.ndim == 2 else got_ref[0, rows]
                out_ref[rows] = bf(f32(kept_ref[rows]) + f32(came))

            chunks(key, body)

        return shift(call(kernel, [block], kept, got)[0], "dp_1", step)

    *blocks, tile = terms(*[[far(0, step)] for step in steps], order=[])
    sent_1 = send(blocks)
    *blocks, tile = terms(*[[lag(0, step), far(1, step)] for step in steps], order=[tile])
    sent_2 = send(blocks)
    *blocks, stored, tile = terms(*[[near(0, step)] for step in steps], own(0), order=[tile])
    blocks, tiles = add(blocks, sent_1, 0)
    sent_3 = send(blocks)
    *blocks, tile = terms(*[[lag(1, step)] for step in steps], order=[tile, *tiles])
    sent_4 = send(blocks)
    *blocks, stored_2, _ = terms(*[[near(1, step)] for step in steps], own(1), order=[tile])
    blocks, _ = add(blocks, sent_2, 2)
    sent_5 = send(blocks)
    outs = [block, ((2, key, LANES), jnp.bfloat16), block]
    came = [sent_3[1], sent_2[-1], sent_2[1], sent_3[-1]]
    four, pair, minus_three = call(outer_kernel, outs, stored, *came)
    pair = shift(pair, "dp_1", 1)
    four = shift(four, "dp_1", -1)
    three = passed(-1, minus_three, four)
    came = [sent_5[1], sent_4[-1], sent_4[1], sent_5[-1]]
    minus_one, two, minus_two, mine = call(inner_kernel, [block] * 4, stored_2, *came)

    ahead = passed(2, two, pair)
    behind = passed(-1, minus_one, passed(-1, minus_two, three))
    return end(samples, mine, ahead, behind, pair)


def end(samples, *terms):
    key = terms[0].shape[0]

    def kernel(*refs):
        def body(rows):
            value = f32(refs[0][rows])
            for ref in refs[1:-1]:
                value = value + f32(ref[rows] if ref.ndim == 2 else ref[1, rows])
            refs[-1][:, rows] = bf(value.T / samples)

        chunks(key, body)

    return call(kernel, [((LANES, key), jnp.bfloat16)], *terms)[0]


def z_first(acts, flipped, samples):
    nx, nz = lax.axis_size("dp_0"), lax.axis_size("dp_1")
    key = flipped.shape[0]
    order = [[2, 1], [-1, 0]]
    block_id = lambda t, half: [(lax.axis_index("dp_0") + d) % nx * nz + t for d in order[half]]
    stored, got = two_way(acts, flipped, "dp_1", block_id, 2)

    def rows_kernel(stored_ref, a1, a2, b1, b2, *outs):
        def body(rows):
            for k, out in enumerate(outs):
                one, two = (a1, a2) if k < 2 else (b1, b2)
                value = f32(stored_ref[k, rows]) + f32(one[k % 2, rows])
                out[rows] = bf(value + f32(two[k % 2, rows]))

        chunks(key, body)

    block = ((key, LANES), jnp.bfloat16)
    *outs, own = call(rows_kernel, [block] * 4, stored, *got[0], *got[1])
    moved = [shift(out, "dp_0", d) for out, d in zip(outs, (2, 1, -1))]
    return end(samples, own, *moved)


def on_device(activations, out_grads, lengths):
    layer_count, example_count, seq_len, model_width = activations.shape
    key_width = out_grads.shape[3]
    total_layers = layer_count * lax.axis_size("section")
    clip_bound = 0.5 * math.sqrt(float(total_layers * seq_len * model_width * key_width))
    acts, grads = activations[0], out_grads[0]
    own = example_norms(acts, grads, lengths)
    pair = partner_sum(own, 0)
    turned, tile = masked_rows(grads, lengths, pair)
    quad = partner_sum(pair, 1, tile)
    stored, tile = on_chip(acts, quad)
    total = partner_sum(quad, 2, tile)
    flipped, norm_ratio = clipped_rows(turned, total, clip_bound)
    samples = float(lax.axis_size(DP) * example_count)
    first = functools.partial(x_first, samples=samples)
    second = functools.partial(z_first, samples=samples)
    mean = lax.cond(lax.axis_index("section") % 2 == 0, first, second, stored, flipped)
    return (mean[None], norm_ratio)


def solution(mesh):
    torus = Mesh(mesh.devices.reshape(4, 8, mesh.shape["section"]), ("dp_0", "dp_1", "section"))
    return jax.shard_map(
        on_device,
        mesh=torus,
        in_specs=(P("section", DP, None, None), P("section", DP, None, None), P(DP)),
        out_specs=(P("section", DP, None), P(DP)),
        check_vma=False,
    )
```

```python
import functools
import math

import jax
import jax.numpy as jnp
from jax import lax
from jax.experimental import pallas as pl
from jax.experimental.pallas import tpu as pltpu
from jax.sharding import Mesh
from jax.sharding import PartitionSpec as P


DP = ("dp_0", "dp_1")
LANES = 128
NORM_STEPS = 2
CHUNK = 256
WHOLE = pl.BlockSpec(memory_space=pltpu.VMEM)


def bf(v):
    return v.astype(jnp.bfloat16)


def f32(v):
    return v.astype(jnp.float32)


def in_hbm(v):
    return pltpu.with_memory_space_constraint(v, pltpu.HBM)


def in_vmem(v):
    return pltpu.with_memory_space_constraint(v, pltpu.VMEM)


def partner_sum(own, level, *order):
    count = lax.axis_size("section")
    moved = lax.ppermute(own, "section", [(i, i ^ 1 << level) for i in range(count)])

    def kernel(own_ref, moved_ref, *refs):
        refs[-1][...] = own_ref[...] + moved_ref[...]

    return call(kernel, [(own.shape, own.dtype)], own, moved, *order)[0]


def chunks(total, body):
    def step(i, _):
        body(pl.ds(pl.multiple_of(i * CHUNK, CHUNK), CHUNK))
        return 0

    lax.fori_loop(0, total // CHUNK, step, 0)


def shift(block, axis, step):
    count = lax.axis_size(axis)
    return lax.ppermute(block, axis, [(i, (i + step) % count) for i in range(count)])


def row_products(left, right):
    return lax.dot_general(left, right, (((1,), (1,)), ((), ())), preferred_element_type=jnp.float32)


def norm_kernel(len_src, act_ref, grad_ref, norm_ref, top_ref, low_ref, len_ref, sem):
    j = pl.program_id(0)
    examples, seq, _ = act_ref.shape
    half = seq // 2
    first = j == 0
    load = pltpu.make_async_copy(len_src, len_ref, sem)

    @pl.when(first)
    def _():
        load.start()

    def gram(e, _):
        acts = act_ref[e]
        top = row_products(acts[:half], acts)
        low = row_products(acts[half:], acts[half:])
        top_ref[e] = top + jnp.where(first, 0.0, top_ref[e])
        low_ref[e] = low + jnp.where(first, 0.0, low_ref[e])
        return 0

    lax.fori_loop(0, examples, gram, 0)

    @pl.when(first)
    def _():
        load.wait()

    def finish(e, _):
        row = lax.broadcasted_iota(jnp.int32, (half, seq), 0)
        col = lax.broadcasted_iota(jnp.int32, (half, seq), 1)
        grads = grad_ref[e]
        size = len_ref[e]
        top = row_products(grads[:half], grads) * top_ref[e]
        low = row_products(grads[half:], grads[half:]) * low_ref[e]
        top = jnp.where((row < size) & (col < size), top, 0.0)
        inner = (row[:, :half] + half < size) & (col[:, :half] + half < size)
        low = jnp.where(inner, low, 0.0)
        total = jnp.sum(top[:, :half]) + 2.0 * jnp.sum(top[:, half:]) + jnp.sum(low)
        norm_ref[e] = jnp.full(norm_ref.shape[1:], total, jnp.float32)
        return 0

    @pl.when(j == pl.num_programs(0) - 1)
    def _():
        lax.fori_loop(0, examples, finish, 0)


def example_norms(acts, grads, lengths):
    examples, seq, width = acts.shape
    key = grads.shape[2]
    tile = width // NORM_STEPS
    half = seq // 2
    return pl.pallas_call(
        norm_kernel,
        grid=(NORM_STEPS,),
        in_specs=[
            pl.BlockSpec(memory_space=pltpu.HBM),
            pl.BlockSpec((examples, seq, tile), lambda j: (0, 0, j)),
            pl.BlockSpec((examples, seq, key), lambda j: (0, 0, 0)),
        ],
        out_specs=WHOLE,
        out_shape=pltpu.VMEM((examples, 8, LANES), jnp.float32),
        scratch_shapes=[
            pltpu.VMEM((examples, half, seq), jnp.float32),
            pltpu.VMEM((examples, half, half), jnp.float32),
            pltpu.SMEM((examples,), jnp.int32),
            pltpu.SemaphoreType.DMA,
        ],
        compiler_params=pltpu.CompilerParams(
            dimension_semantics=("arbitrary",), vmem_limit_bytes=30 << 20
        ),
        name="example_norms",
    )(in_hbm(lengths), in_hbm(acts), in_hbm(grads))


def on_chip(acts, order):
    def kernel(acts_ref, order_ref, out_ref, tile_ref, sem):
        tile_ref[...] = jnp.zeros_like(tile_ref)
        copy = pltpu.make_async_copy(acts_ref, out_ref, sem)
        copy.start()
        copy.wait()

    return pl.pallas_call(
        kernel,
        in_specs=[pl.BlockSpec(memory_space=pltpu.HBM), WHOLE],
        out_specs=[WHOLE, WHOLE],
        out_shape=[
            pltpu.VMEM(acts.shape, acts.dtype),
            pltpu.VMEM((8, LANES), jnp.float32),
        ],
        scratch_shapes=[pltpu.SemaphoreType.DMA],
        compiler_params=pltpu.CompilerParams(vmem_limit_bytes=2 << 20),
        name="on_chip",
    )(in_hbm(acts), in_vmem(order))


def masked_rows(grads, lengths, order):
    examples, seq, key = grads.shape

    def kernel(len_ref, grad_ref, order_ref, flip_ref, tile_ref):
        tile_ref[...] = jnp.zeros_like(tile_ref)

        def turn(e, _):
            token = lax.broadcasted_iota(jnp.int32, (seq, key), 0)
            masked = jnp.where(token < len_ref[e], f32(grad_ref[e]), 0.0)
            flip_ref[:, pl.ds(pl.multiple_of(e * seq, seq), seq)] = bf(masked).T
            return 0

        lax.fori_loop(0, examples, turn, 0)

    return pl.pallas_call(
        kernel,
        in_specs=[pl.BlockSpec(memory_space=pltpu.SMEM), WHOLE, WHOLE],
        out_specs=[WHOLE, WHOLE],
        out_shape=[
            pltpu.VMEM((key, examples * seq), jnp.bfloat16),
            pltpu.VMEM((8, LANES), jnp.float32),
        ],
        compiler_params=pltpu.CompilerParams(vmem_limit_bytes=16 << 20),
        name="masked_rows",
    )(lengths, grads, in_vmem(order))


def clipped_rows(flipped, total, bound):
    examples = total.shape[0]
    seq = flipped.shape[1] // examples

    def kernel(total_ref, flip_ref, out_ref, ratio_ref):
        clips = []
        for e in range(examples):
            ratio = jnp.sqrt(total_ref[e]) / bound
            ratio_ref[e] = ratio[0, 0]
            clips.append((1.0 / jnp.maximum(ratio, 1.0))[:1, :1])

        def body(rows):
            for e in range(examples):
                part = (rows, slice(e * seq, (e + 1) * seq))
                out_ref[part] = bf(f32(flip_ref[part]) * clips[e])

        chunks(flipped.shape[0], body)

    return pl.pallas_call(
        kernel,
        in_specs=[WHOLE, WHOLE],
        out_specs=[WHOLE, pl.BlockSpec(memory_space=pltpu.SMEM)],
        out_shape=[
            pltpu.VMEM(flipped.shape, flipped.dtype),
            jax.ShapeDtypeStruct((examples,), jnp.float32),
        ],
        compiler_params=pltpu.CompilerParams(vmem_limit_bytes=8 << 20),
        name="clipped_rows",
    )(in_vmem(total), in_vmem(flipped))


def pieces(acts, flipped, ids, outs, step, order):
    examples, seq, _ = acts.shape
    key = flipped.shape[0]

    def kernel(acts_ref, flip_ref, *refs):
        refs = refs[len(order) :]
        refs[-1][...] = jnp.zeros_like(refs[-1])
        blocks = ids()

        def strip(k):
            cols = pl.ds(pl.multiple_of(blocks[k] * LANES, LANES), LANES)
            return acts_ref[:, :, cols].reshape(examples * seq, LANES)

        places = [(out, at) for out, size in zip(refs[:-1], outs) for at in range(size)]

        def rows_of(i, _):
            rows = pl.ds(pl.multiple_of(i * step, step), step)
            for first in range(0, len(places), 4):
                some = range(first, min(first + 4, len(places)))
                block = jnp.concatenate([strip(k) for k in some], 1)
                value = jnp.dot(flip_ref[rows, :], block, preferred_element_type=jnp.float32)
                for q, k in enumerate(some):
                    out, at = places[k]
                    out[at, rows] = bf(value[:, q * LANES : (q + 1) * LANES])
            return 0

        lax.fori_loop(0, key // step, rows_of, 0)

    return pl.pallas_call(
        kernel,
        in_specs=[WHOLE] * (2 + len(order)),
        out_specs=[WHOLE] * (len(outs) + 1),
        out_shape=[pltpu.VMEM((size, key, LANES), jnp.bfloat16) for size in outs]
        + [pltpu.VMEM((8, LANES), jnp.float32)],
        compiler_params=pltpu.CompilerParams(vmem_limit_bytes=12 << 20),
        name="terms",
    )(*[in_vmem(v) for v in (acts, flipped, *order)])


def call(kernel, outs, *args, space=pltpu.VMEM):
    return pl.pallas_call(
        kernel,
        in_specs=[WHOLE] * len(args),
        out_specs=[WHOLE] * len(outs),
        out_shape=[space(shape, dtype) for shape, dtype in outs],
        compiler_params=pltpu.CompilerParams(vmem_limit_bytes=8 << 20),
    )(*[in_vmem(a) for a in args])


def plus(stored, got, skip=0):
    def kernel(stored_ref, got_ref, out_ref, order_ref):
        order_ref[...] = jnp.zeros_like(order_ref)

        def body(rows):
            for k in range(out_ref.shape[0]):
                out_ref[k, rows] = bf(f32(stored_ref[k, rows]) + f32(got_ref[skip + k, rows]))

        chunks(out_ref.shape[1], body)

    outs = [(stored.shape, stored.dtype), ((8, LANES), jnp.float32)]
    return call(kernel, outs, stored, got)


def two_way(acts, flipped, axis, block_id, size):
    count = lax.axis_size(axis)
    far = count // 2
    sent, order = {}, []
    for slot in range(count - 1):
        routes = [(step, slot % 2 if step == 1 else 1 - slot % 2) for step in (1, -1)]
        hops = far - (slot + 1) // 2
        wanted, outs = [(step * hops, half) for step, half in routes], [size, size]
        if slot == count - 2:
            wanted, outs = wanted + [(0, 0), (0, 1)], outs + [2 * size]

        def ids(wanted=wanted):
            index = lax.axis_index(axis)
            return [k for away, half in wanted for k in block_id((index + away) % count, half)]

        *terms, tile = pieces(acts, flipped, ids, outs, 256, order)
        order = [tile]
        for route, term in zip(routes, terms):
            if slot > 1:
                term, tile = plus(term, sent[route])
                order.append(tile)
            sent[route] = shift(term, axis, route[0])
    return terms[2], [[sent[step, half] for step in (1, -1)] for half in (0, 1)]


def x_first(acts, flipped, samples):
    nx, nz = lax.axis_size("dp_0"), lax.axis_size("dp_1")
    key = flipped.shape[0]
    block = ((key, LANES), jnp.bfloat16)

    offsets = {(0, 0): [4, 3], (0, 1): [1, -3], (1, 0): [-1, 2], (1, 1): [-2, 0]}
    steps = (1, -1)

    def terms(*wanted, order):
        def ids():
            x, z = lax.axis_index("dp_0"), lax.axis_index("dp_1")
            return [
                (x + away) % nx * nz + (z + d) % nz
                for parts in wanted
                for batch, half, away in parts
                for d in offsets[batch, half]
            ]

        outs = [2 * len(parts) for parts in wanted]
        return pieces(acts, flipped, ids, outs, 256, order)

    lead = {1: 0, -1: 1}
    far = lambda batch, step: (batch, lead[step], 2 * step)
    lag = lambda batch, step: (batch, 1 - lead[step], step)
    near = lambda batch, step: (batch, lead[step], step)
    own = lambda batch: [(batch, 0, 0), (batch, 1, 0)]

    def send(blocks):
        return {step: shift(block, "dp_0", step) for step, block in zip(steps, blocks)}

    def add(blocks, got, skip):
        outs = [plus(block, got[step], skip) for step, block in zip(steps, blocks)]
        return [out for out, _ in outs], [tile for _, tile in outs]

    def row(refs, k, rows):
        stored, a1, a2, b1, b2 = refs
        one, two = (a1, a2) if k < 2 else (b1, b2)
        return bf(f32(stored[k, rows]) + f32(one[k % 2, rows]) + f32(two[k % 2, rows]))

    def outer_kernel(*refs):
        four, pair, minus_three = refs[5:]

        def body(rows):
            four[rows] = row(refs[:5], 0, rows)
            pair[0, rows] = row(refs[:5], 1, rows)
            pair[1, rows] = row(refs[:5], 2, rows)
            minus_three[rows] = row(refs[:5], 3, rows)

        chunks(key, body)

    def inner_kernel(*refs):
        outs = refs[5:]

        def body(rows):
            for k, out in enumerate(outs):
                out[rows] = row(refs[:5], k, rows)

        chunks(key, body)

    def passed(step, kept, got):
        def kernel(kept_ref, got_ref, out_ref):
            def body(rows):
                came = got_ref[rows] if got_ref.ndim == 2 else got_ref[0, rows]
                out_ref[rows] = bf(f32(kept_ref[rows]) + f32(came))

            chunks(key, body)

        return shift(call(kernel, [block], kept, got)[0], "dp_1", step)

    *blocks, tile = terms(*[[far(0, step)] for step in steps], order=[])
    sent_1 = send(blocks)
    *blocks, tile = terms(*[[lag(0, step), far(1, step)] for step in steps], order=[tile])
    sent_2 = send(blocks)
    *blocks, stored, tile = terms(*[[near(0, step)] for step in steps], own(0), order=[tile])
    blocks, tiles = add(blocks, sent_1, 0)
    sent_3 = send(blocks)
    *blocks, tile = terms(*[[lag(1, step)] for step in steps], order=[tile, *tiles])
    sent_4 = send(blocks)
    *blocks, stored_2, _ = terms(*[[near(1, step)] for step in steps], own(1), order=[tile])
    blocks, _ = add(blocks, sent_2, 2)
    sent_5 = send(blocks)
    outs = [block, ((2, key, LANES), jnp.bfloat16), block]
    came = [sent_3[1], sent_2[-1], sent_2[1], sent_3[-1]]
    four, pair, minus_three = call(outer_kernel, outs, stored, *came)
    pair = shift(pair, "dp_1", 1)
    four = shift(four, "dp_1", -1)
    three = passed(-1, minus_three, four)
    came = [sent_5[1], sent_4[-1], sent_4[1], sent_5[-1]]
    minus_one, two, minus_two, mine = call(inner_kernel, [block] * 4, stored_2, *came)

    ahead = passed(2, two, pair)
    behind = passed(-1, minus_one, passed(-1, minus_two, three))
    return end(samples, mine, ahead, behind, pair)


def end(samples, *terms):
    key = terms[0].shape[0]

    def kernel(*refs):
        def body(rows):
            value = f32(refs[0][rows])
            for ref in refs[1:-1]:
                value = value + f32(ref[rows] if ref.ndim == 2 else ref[1, rows])
            refs[-1][:, rows] = bf(value.T / samples)

        chunks(key, body)

    return call(kernel, [((LANES, key), jnp.bfloat16)], *terms)[0]


def z_first(acts, flipped, samples):
    nx, nz = lax.axis_size("dp_0"), lax.axis_size("dp_1")
    key = flipped.shape[0]
    order = [[2, 1], [-1, 0]]
    block_id = lambda t, half: [(lax.axis_index("dp_0") + d) % nx * nz + t for d in order[half]]
    stored, got = two_way(acts, flipped, "dp_1", block_id, 2)

    def rows_kernel(stored_ref, a1, a2, b1, b2, *outs):
        def body(rows):
            for k, out in enumerate(outs):
                one, two = (a1, a2) if k < 2 else (b1, b2)
                value = f32(stored_ref[k, rows]) + f32(one[k % 2, rows])
                out[rows] = bf(value + f32(two[k % 2, rows]))

        chunks(key, body)

    block = ((key, LANES), jnp.bfloat16)
    *outs, own = call(rows_kernel, [block] * 4, stored, *got[0], *got[1])
    moved = [shift(out, "dp_0", d) for out, d in zip(outs, (2, 1, -1))]
    return end(samples, own, *moved)


def on_device(activations, out_grads, lengths):
    layer_count, example_count, seq_len, model_width = activations.shape
    key_width = out_grads.shape[3]
    total_layers = layer_count * lax.axis_size("section")
    clip_bound = 0.5 * math.sqrt(float(total_layers * seq_len * model_width * key_width))
    acts, grads = activations[0], out_grads[0]
    own = example_norms(acts, grads, lengths)
    pair = partner_sum(own, 0)
    turned, tile = masked_rows(grads, lengths, pair)
    quad = partner_sum(pair, 1, tile)
    stored, tile = on_chip(acts, quad)
    total = partner_sum(quad, 2, tile)
    flipped, norm_ratio = clipped_rows(turned, total, clip_bound)
    samples = float(lax.axis_size(DP) * example_count)
    first = functools.partial(x_first, samples=samples)
    second = functools.partial(z_first, samples=samples)
    mean = lax.cond(lax.axis_index("section") % 2 == 0, first, second, stored, flipped)
    return (mean[None], norm_ratio)


def solution(mesh):
    torus = Mesh(mesh.devices.reshape(4, 8, mesh.shape["section"]), ("dp_0", "dp_1", "section"))
    return jax.shard_map(
        on_device,
        mesh=torus,
        in_specs=(P("section", DP, None, None), P("section", DP, None, None), P(DP)),
        out_specs=(P("section", DP, None), P(DP)),
        check_vma=False,
    )
```
